32 devices in a mesh: mp: 8 (over z, y), dp: 4 (over x, core).
Axes of the slice: x: 2, y: 2, z: 4, core: 2. Of those that a mesh axis runs over, the one named last changes fastest.
Arguments:
- features: bfloat16 [32, 4, 4, 512], P(('dp', 'mp')), may hold values from 0 to 2
- labels: int32 [32], P('dp'), may hold values from 0 to 9
- subset_ids: int32 [8], P('mp'), may hold values from 0 to 255
- conv1_weight: bfloat16 [8, 9, 512, 512], P('mp'), may hold values from -0.09375 to 0.09375
- conv2_weight: bfloat16 [8, 9, 512, 512], P('mp'), may hold values from -0.09375 to 0.09375
- head_weight: float32 [8, 512, 10], P('mp'), may hold values from -0.25 to 0.25
Outputs:
- datamodel: float32 [32, 256], P(('dp', 'mp'))
- margin_mean: float32 [32], P(('dp', 'mp'))
- margin_norm: float32 [32], P(('dp', 'mp'))
The draws below stay inside these ranges and needn't reach their ends.
All inputs are finite; a program needn't handle non-finite values.
Results may differ from the reference program's by a relative error of at most 0.00077.
Values may be sent and summed in bfloat16 or wider, within the bound.
A program may use at most 128 MiB of HBM per device.

```python
import jax
import jax.numpy as jnp
from jax import lax

C = 512
CLASSES = 10
SIDE = 4
SUBSETS = 256
TARGETS = 32
MODELS = 8


def with_ends(entries, own_key, low, high):
    dims = entries.shape
    spot = [jax.random.randint(jax.random.fold_in(own_key, axis), (), 0, dims[axis]) for axis in range(len(dims))]
    entries = entries.at[tuple(spot)].set(low)
    longest = dims.index(max(dims))
    spot[longest] = (spot[longest] + 1) % dims[longest]
    return entries.at[tuple(spot)].set(high)


def block_levels(key, shape, cuts, smallest, top_value):
    level = 1.0
    for dim, shards_of in cuts:
        draws = jax.random.uniform(jax.random.fold_in(jax.random.fold_in(key, 6), dim), (shards_of,), jnp.float32, smallest / len(cuts), top_value / len(cuts))
        level = level * jnp.repeat(jnp.exp(draws), shape[dim] // shards_of).reshape((-1,) + (1,) * (len(shape) - 1 - dim))
    return level


def bell_draw(stream_key, shape, deviation, reach, pieces=(), kind=jnp.bfloat16):
    drawn = deviation * jax.random.normal(stream_key, shape, jnp.float32)
    if pieces:
        drawn = drawn * block_levels(stream_key, shape, pieces, -0.22, 0.18)
    return jnp.clip(drawn, -reach, reach).astype(kind)


def setup_inputs(seed: int = 0) -> dict:
    streams_of = jax.random.split(jax.random.key(seed), 7)
    features = jnp.clip(2.0 * jax.random.uniform(streams_of[0], (TARGETS, SIDE, SIDE, C), jnp.float32) ** block_levels(streams_of[0], (TARGETS, SIDE, SIDE, C), ((0, 32),), -0.2, 0.2), 0.0, 2.0).astype(jnp.bfloat16)
    labels = with_ends(jax.random.randint(streams_of[1], (TARGETS,), 0, CLASSES), jax.random.fold_in(streams_of[1], 1), 0, CLASSES - 1).astype(jnp.int32)
    subset_ids = with_ends(jax.random.randint(streams_of[2], (MODELS,), 0, SUBSETS), jax.random.fold_in(streams_of[2], 1), 0, SUBSETS - 1).astype(jnp.int32)
    conv1_weight = bell_draw(streams_of[3], (MODELS, 9, C, C), (9 * C) ** -0.5, 0.09375, ((0, 8),))
    conv2_weight = bell_draw(streams_of[4], (MODELS, 9, C, C), (9 * C) ** -0.5, 0.09375, ((0, 8),))
    head_weight = bell_draw(streams_of[5], (MODELS, C, CLASSES), C ** -0.5, 0.25, ((0, 8),), jnp.float32)
    return {"features": features, "labels": labels, "subset_ids": subset_ids, "conv1_weight": conv1_weight, "conv2_weight": conv2_weight, "head_weight": head_weight}


def convolve(grid, kernel):
    batch = grid.shape[0]
    width = grid.shape[1]
    chans = grid.shape[3]
    padded = jnp.pad(grid, ((0, 0), (1, 1), (1, 1), (0, 0)))
    result = jnp.zeros((batch * width * width, kernel.shape[2]), jnp.float32)
    for offset in range(9):
        row_off, col_off = divmod(offset, 3)
        shifted = padded[:, row_off:row_off + width, col_off:col_off + width, :].reshape(batch * width * width, chans)
        result = result + jnp.dot(shifted, kernel[offset], preferred_element_type=jnp.float32)
    return result

def margins_of(grid, first_kernel, second_kernel, head, target_labels):
    batch = grid.shape[0]
    width = grid.shape[1]
    chans = grid.shape[3]
    hidden = jax.nn.relu(convolve(grid, first_kernel)).astype(jnp.bfloat16).reshape(batch, width, width, chans)
    branch = jax.nn.relu(convolve(hidden, second_kernel))
    blocked = grid.astype(jnp.float32).reshape(batch * width * width, chans) + branch
    pooled = lax.optimization_barrier(jnp.max(blocked.reshape(batch, width * width, chans), axis=1))
    logits = jnp.dot(pooled, head, precision=lax.Precision.HIGHEST, preferred_element_type=jnp.float32)
    classes = jnp.arange(head.shape[1], dtype=jnp.int32)[None, :]
    chosen = classes == target_labels[:, None]
    correct = lax.optimization_barrier(jnp.sum(jnp.where(chosen, logits, 0.0), axis=1))
    rival = lax.optimization_barrier(jnp.max(jnp.where(chosen, -1e+30, logits), axis=1))
    return correct - rival

def reference(features, labels, subset_ids, conv1_weight, conv2_weight, head_weight):

    def single(weights):
        return margins_of(features, weights[0], weights[1], weights[2], labels)
    margin = lax.map(single, (conv1_weight, conv2_weight, head_weight))
    model_count = margin.shape[0]
    margin_mean = lax.optimization_barrier(jnp.sum(margin, axis=0)) / model_count
    centred = margin - margin_mean[None, :]
    margin_norm = jnp.sqrt(1.0 + lax.optimization_barrier(jnp.sum(centred * centred, axis=0)) / model_count)
    scaled = centred / margin_norm[None, :]
    onehot = (subset_ids[:, None] == jnp.arange(SUBSETS, dtype=jnp.int32)[None, :]).astype(jnp.float32)
    datamodel = jnp.dot(scaled.T, onehot, precision=lax.Precision.HIGHEST, preferred_element_type=jnp.float32)
    return (datamodel, margin_mean, margin_norm)
```

```python
import functools

import jax
import jax.numpy as jnp
from jax import lax
from jax.experimental import pallas as pl
from jax.experimental.pallas import tpu as pltpu
from jax.sharding import PartitionSpec as P

SUBSETS = 256
GROUP = 8
LANES = 128
MESH = pl.DeviceIdType.MESH


def kernel(
    n, feat_ref, labels_ref, ids_ref, w1_ref, w2_ref, head_ref,
    data_ref, mean_ref, norm_ref,
    gathered, w1, w2, head, lhs, msg, got,
    own_sem, w1_sem, w2_sem, head_sem, fsend, frecv, msend, mrecv,
):
    me = lax.axis_index("mp")
    width = feat_ref.shape[1]
    chans = feat_ref.shape[3]
    spots = width * width
    rows = GROUP * spots
    offsets = w1_ref.shape[1]
    classes = head_ref.shape[0]

    own = pltpu.make_async_copy(feat_ref.at[0], gathered.at[me], own_sem)
    own.start()
    w1_copies = [
        pltpu.make_async_copy(w1_ref.at[0, o], w1.at[o], w1_sem.at[o]) for o in range(offsets)
    ]
    w2_copies = [
        pltpu.make_async_copy(w2_ref.at[0, o], w2.at[o], w2_sem.at[o]) for o in range(offsets)
    ]
    head_copy = pltpu.make_async_copy(head_ref, head, head_sem)

    peers = [lax.rem(me + j, n) for j in range(1, n)]
    barrier = pltpu.get_barrier_semaphore()
    for peer in peers:
        pl.semaphore_signal(barrier, inc=1, device_id={"mp": peer}, device_id_type=MESH)
    for copy in w1_copies:
        copy.start()
    for copy in w2_copies:
        copy.start()
    head_copy.start()

    r = lax.broadcasted_iota(jnp.int32, (rows, rows), 0)
    c = lax.broadcasted_iota(jnp.int32, (rows, rows), 1)
    source = lax.rem(r, GROUP) * spots + lax.div(r, GROUP)
    reorder = jnp.where(c == source, 1.0, 0.0).astype(jnp.bfloat16)
    sub = lax.broadcasted_iota(jnp.int32, (GROUP, 1), 0)
    identity = ids_ref[0].astype(jnp.float32)
    for t in range(n):
        msg[t, 1:2, :] = jnp.full((1, LANES), identity, jnp.float32)

    own.wait()
    pl.semaphore_wait(barrier, n - 1)
    feature_sends = []
    for j, peer in enumerate(peers):
        copy = pltpu.make_async_remote_copy(
            src_ref=gathered.at[me], dst_ref=gathered.at[me],
            send_sem=fsend.at[j], recv_sem=frecv.at[me],
            device_id={"mp": peer}, device_id_type=MESH,
        )
        copy.start()
        feature_sends.append(copy)

    for copy in w1_copies:
        copy.wait()
    for copy in w2_copies:
        copy.wait()
    head_copy.wait()
    for peer in peers:
        pltpu.make_async_remote_copy(
            src_ref=gathered.at[peer], dst_ref=gathered.at[peer],
            send_sem=fsend.at[0], recv_sem=frecv.at[peer],
            device_id={"mp": peer}, device_id_type=MESH,
        ).wait_recv()

    def convolve(grid, kernel_ref):
        blank = jnp.zeros((GROUP, chans), jnp.float32)
        for o in range(offsets):
            dy, dx = o // 3 - 1, o % 3 - 1
            blocks = []
            for y in range(width):
                for x in range(width):
                    inside = 0 <= y + dy < width and 0 <= x + dx < width
                    q = ((y + dy) * width + x + dx) * GROUP
                    blocks.append(grid[q : q + GROUP] if inside else blank)
            lhs[:, o * chans : (o + 1) * chans] = jnp.concatenate(blocks, 0).astype(jnp.bfloat16)
        return jnp.dot(
            lhs[...],
            kernel_ref[...].reshape(offsets * chans, chans),
            preferred_element_type=jnp.float32,
        )

    def group(first):
        raw = gathered[pl.ds(first, GROUP)].astype(jnp.float32).reshape(rows, chans)
        grid = jnp.dot(reorder, raw.astype(jnp.bfloat16), preferred_element_type=jnp.float32)
        hidden = jnp.maximum(convolve(grid, w1), 0.0)
        block = grid + jnp.maximum(convolve(hidden, w2), 0.0)
        pooled = block[:GROUP]
        for p in range(1, spots):
            pooled = jnp.maximum(pooled, block[p * GROUP : (p + 1) * GROUP])
        label = jnp.zeros((GROUP, 1), jnp.int32)
        for t in range(GROUP):
            label = jnp.where(sub == t, labels_ref[first + t], label)
        correct = jnp.zeros((GROUP, 1), jnp.float32)
        rival = jnp.full((GROUP, 1), -1e30, jnp.float32)
        for k in range(classes):
            logit = jnp.sum(pooled * head[k], axis=1, keepdims=True)
            correct = jnp.where(label == k, logit, correct)
            rival = jnp.where(label == k, rival, jnp.maximum(rival, logit))
        margin = jnp.broadcast_to(correct - rival, (GROUP, LANES))
        for t in range(GROUP):
            msg[first + t, 0:1, :] = margin[t : t + 1]

    if n == GROUP:
        group(0)
    else:
        pl.loop(0, n // GROUP)(lambda g: group(g * GROUP))

    margin_sends = []
    for j, peer in enumerate(peers):
        copy = pltpu.make_async_remote_copy(
            src_ref=msg.at[peer], dst_ref=got.at[me],
            send_sem=msend.at[j], recv_sem=mrecv.at[me],
            device_id={"mp": peer}, device_id_type=MESH,
        )
        copy.start()
        margin_sends.append(copy)
    got[me] = msg[me]
    for copy in feature_sends:
        copy.wait_send()
    for copy in margin_sends:
        copy.wait_send()
    for peer in peers:
        pltpu.make_async_remote_copy(
            src_ref=msg.at[peer], dst_ref=got.at[peer],
            send_sem=msend.at[0], recv_sem=mrecv.at[peer],
            device_id={"mp": peer}, device_id_type=MESH,
        ).wait_recv()

    total = got[0, 0:1, :]
    for m in range(1, n):
        total = total + got[m, 0:1, :]
    mean = total / n
    spread = jnp.zeros_like(mean)
    for m in range(n):
        centred = got[m, 0:1, :] - mean
        spread = spread + centred * centred
    norm = jnp.sqrt(1.0 + spread / n)
    lane = lax.broadcasted_iota(jnp.int32, (1, LANES), 1).astype(jnp.float32)
    for start in range(0, SUBSETS, LANES):
        acc = jnp.zeros((1, LANES), jnp.float32)
        for m in range(n):
            scaled = (got[m, 0:1, :] - mean) / norm
            acc = acc + jnp.where(got[m, 1:2, :] == lane + start, scaled, 0.0)
        data_ref[:, start : start + LANES] = acc
    mean_ref[...] = mean[0, :1]
    norm_ref[...] = norm[0, :1]


def shards(n, features, labels, subset_ids, conv1_weight, conv2_weight, head_weight):
    width, chans = features.shape[1], features.shape[3]
    offsets = conv1_weight.shape[1]
    assert features.shape[0] == 1 and conv1_weight.shape[0] == 1 and n % GROUP == 0
    head = jnp.transpose(head_weight, (2, 0, 1))
    anywhere = pl.BlockSpec(memory_space=pl.ANY)
    smem = pl.BlockSpec(memory_space=pltpu.SMEM)
    vmem = pl.BlockSpec(memory_space=pltpu.VMEM)
    return pl.pallas_call(
        functools.partial(kernel, n),
        out_shape=(
            jax.ShapeDtypeStruct((1, SUBSETS), jnp.float32),
            jax.ShapeDtypeStruct((1,), jnp.float32),
            jax.ShapeDtypeStruct((1,), jnp.float32),
        ),
        in_specs=[anywhere, smem, smem, anywhere, anywhere, anywhere],
        out_specs=(vmem, vmem, vmem),
        scratch_shapes=[
            pltpu.VMEM((n, width, width, chans), features.dtype),
            pltpu.VMEM(conv1_weight.shape[1:], conv1_weight.dtype),
            pltpu.VMEM(conv2_weight.shape[1:], conv2_weight.dtype),
            pltpu.VMEM(head.shape, head.dtype),
            pltpu.VMEM((GROUP * width * width, offsets * chans), features.dtype),
            pltpu.VMEM((n, 2, LANES), jnp.float32),
            pltpu.VMEM((n, 2, LANES), jnp.float32),
            pltpu.SemaphoreType.DMA,
            pltpu.SemaphoreType.DMA((offsets,)),
            pltpu.SemaphoreType.DMA((offsets,)),
            pltpu.SemaphoreType.DMA,
            pltpu.SemaphoreType.DMA((n,)),
            pltpu.SemaphoreType.DMA((n,)),
            pltpu.SemaphoreType.DMA((n,)),
            pltpu.SemaphoreType.DMA((n,)),
        ],
        compiler_params=pltpu.CompilerParams(
            collective_id=0, has_side_effects=True, vmem_limit_bytes=60 * 1024 * 1024
        ),
    )(features, labels, subset_ids, conv1_weight, conv2_weight, head)


def solution(mesh):
    in_specs = (
        P(("dp", "mp"), None, None, None),
        P("dp"),
        P("mp"),
        P("mp", None, None, None),
        P("mp", None, None, None),
        P("mp", None, None),
    )
    out_specs = (P(("dp", "mp"), None), P(("dp", "mp")), P(("dp", "mp")))
    return jax.shard_map(
        functools.partial(shards, mesh.shape["mp"]),
        mesh=mesh, in_specs=in_specs, out_specs=out_specs, check_vma=False,
    )
```

```python
import functools

import jax
import jax.numpy as jnp
from jax import lax
from jax.experimental import pallas as pl
from jax.experimental.pallas import tpu as pltpu
from jax.sharding import PartitionSpec as P

SUBSETS = 256
GROUP = 8
LANES = 128
MESH = pl.DeviceIdType.MESH


def kernel(
    n, feat_ref, labels_ref, ids_ref, w1_ref, w2_ref, head_ref,
    data_ref, mean_ref, norm_ref,
    gathered, labels, ids, w1, w2, head, lhs, msg, got,
    small_sem, own_sem, w1_sem, w2_sem, head_sem, fsend, frecv, msend, mrecv,
):
    me = lax.axis_index("mp")
    width = feat_ref.shape[1]
    chans = feat_ref.shape[3]
    spots = width * width
    rows = GROUP * spots
    offsets = w1_ref.shape[1]
    classes = head_ref.shape[0]

    own = pltpu.make_async_copy(feat_ref.at[0], gathered.at[me], own_sem)
    own.start()
    small_copies = [
        pltpu.make_async_copy(labels_ref, labels, small_sem.at[0]),
        pltpu.make_async_copy(ids_ref, ids, small_sem.at[1]),
    ]
    for copy in small_copies:
        copy.start()
    w1_copies = [
        pltpu.make_async_copy(w1_ref.at[0, o], w1.at[o], w1_sem.at[o]) for o in range(offsets)
    ]
    w2_copies = [
        pltpu.make_async_copy(w2_ref.at[0, o], w2.at[o], w2_sem.at[o]) for o in range(offsets)
    ]
    head_copy = pltpu.make_async_copy(head_ref, head, head_sem)

    peers = [lax.rem(me + j, n) for j in range(1, n)]
    barrier = pltpu.get_barrier_semaphore()
    for peer in peers:
        pl.semaphore_signal(barrier, inc=1, device_id={"mp": peer}, device_id_type=MESH)
    for copy in w1_copies:
        copy.start()
    for copy in w2_copies:
        copy.start()
    head_copy.start()

    r = lax.broadcasted_iota(jnp.int32, (rows, rows), 0)
    c = lax.broadcasted_iota(jnp.int32, (rows, rows), 1)
    source = lax.rem(r, GROUP) * spots + lax.div(r, GROUP)
    reorder = jnp.where(c == source, 1.0, 0.0).astype(jnp.bfloat16)
    sub = lax.broadcasted_iota(jnp.int32, (GROUP, 1), 0)
    for copy in small_copies:
        copy.wait()
    identity = ids[0].astype(jnp.float32)
    for t in range(n):
        msg[t, 1:2, :] = jnp.full((1, LANES), identity, jnp.float32)

    own.wait()
    pl.semaphore_wait(barrier, n - 1)
    feature_sends = []
    for j, peer in enumerate(peers):
        copy = pltpu.make_async_remote_copy(
            src_ref=gathered.at[me], dst_ref=gathered.at[me],
            send_sem=fsend.at[j], recv_sem=frecv.at[me],
            device_id={"mp": peer}, device_id_type=MESH,
        )
        copy.start()
        feature_sends.append(copy)

    for copy in w1_copies:
        copy.wait()
    for copy in w2_copies:
        copy.wait()
    head_copy.wait()
    for peer in peers:
        pltpu.make_async_remote_copy(
            src_ref=gathered.at[peer], dst_ref=gathered.at[peer],
            send_sem=fsend.at[0], recv_sem=frecv.at[peer],
            device_id={"mp": peer}, device_id_type=MESH,
        ).wait_recv()

    def convolve(grid, kernel_ref):
        blank = jnp.zeros((GROUP, chans), jnp.float32)
        for o in range(offsets):
            dy, dx = o // 3 - 1, o % 3 - 1
            blocks = []
            for y in range(width):
                for x in range(width):
                    inside = 0 <= y + dy < width and 0 <= x + dx < width
                    q = ((y + dy) * width + x + dx) * GROUP
                    blocks.append(grid[q : q + GROUP] if inside else blank)
            lhs[:, o * chans : (o + 1) * chans] = jnp.concatenate(blocks, 0).astype(jnp.bfloat16)
        return jnp.dot(
            lhs[...],
            kernel_ref[...].reshape(offsets * chans, chans),
            preferred_element_type=jnp.float32,
        )

    def group(first):
        raw = gathered[pl.ds(first, GROUP)].astype(jnp.float32).reshape(rows, chans)
        grid = jnp.dot(reorder, raw.astype(jnp.bfloat16), preferred_element_type=jnp.float32)
        hidden = jnp.maximum(convolve(grid, w1), 0.0)
        block = grid + jnp.maximum(convolve(hidden, w2), 0.0)
        pooled = block[:GROUP]
        for p in range(1, spots):
            pooled = jnp.maximum(pooled, block[p * GROUP : (p + 1) * GROUP])
        label = jnp.zeros((GROUP, 1), jnp.int32)
        for t in range(GROUP):
            label = jnp.where(sub == t, labels[first + t], label)
        correct = jnp.zeros((GROUP, 1), jnp.float32)
        rival = jnp.full((GROUP, 1), -1e30, jnp.float32)
        for k in range(classes):
            logit = jnp.sum(pooled * head[k], axis=1, keepdims=True)
            correct = jnp.where(label == k, logit, correct)
            rival = jnp.where(label == k, rival, jnp.maximum(rival, logit))
        margin = jnp.broadcast_to(correct - rival, (GROUP, LANES))
        for t in range(GROUP):
            msg[first + t, 0:1, :] = margin[t : t + 1]

    if n == GROUP:
        group(0)
    else:
        pl.loop(0, n // GROUP)(lambda g: group(g * GROUP))

    margin_sends = []
    for j, peer in enumerate(peers):
        copy = pltpu.make_async_remote_copy(
            src_ref=msg.at[peer], dst_ref=got.at[me],
            send_sem=msend.at[j], recv_sem=mrecv.at[me],
            device_id={"mp": peer}, device_id_type=MESH,
        )
        copy.start()
        margin_sends.append(copy)
    got[me] = msg[me]
    for copy in feature_sends:
        copy.wait_send()
    for copy in margin_sends:
        copy.wait_send()
    for peer in peers:
        pltpu.make_async_remote_copy(
            src_ref=msg.at[peer], dst_ref=got.at[peer],
            send_sem=msend.at[0], recv_sem=mrecv.at[peer],
            device_id={"mp": peer}, device_id_type=MESH,
        ).wait_recv()

    total = got[0, 0:1, :]
    for m in range(1, n):
        total = total + got[m, 0:1, :]
    mean = total / n
    spread = jnp.zeros_like(mean)
    for m in range(n):
        centred = got[m, 0:1, :] - mean
        spread = spread + centred * centred
    norm = jnp.sqrt(1.0 + spread / n)
    lane = lax.broadcasted_iota(jnp.int32, (1, LANES), 1).astype(jnp.float32)
    for start in range(0, SUBSETS, LANES):
        acc = jnp.zeros((1, LANES), jnp.float32)
        for m in range(n):
            scaled = (got[m, 0:1, :] - mean) / norm
            acc = acc + jnp.where(got[m, 1:2, :] == lane + start, scaled, 0.0)
        data_ref[:, start : start + LANES] = acc
    mean_ref[...] = mean[0, :1]
    norm_ref[...] = norm[0, :1]


def shards(n, features, labels, subset_ids, conv1_weight, conv2_weight, head_weight):
    width, chans = features.shape[1], features.shape[3]
    offsets = conv1_weight.shape[1]
    assert features.shape[0] == 1 and conv1_weight.shape[0] == 1 and n % GROUP == 0
    head = jnp.transpose(head_weight, (2, 0, 1))
    anywhere = pl.BlockSpec(memory_space=pl.ANY)
    hbm = pl.BlockSpec(memory_space=pltpu.HBM)
    vmem = pl.BlockSpec(memory_space=pltpu.VMEM)
    return pl.pallas_call(
        functools.partial(kernel, n),
        out_shape=(
            pltpu.VMEM((1, SUBSETS), jnp.float32),
            pltpu.VMEM((1,), jnp.float32),
            pltpu.VMEM((1,), jnp.float32),
        ),
        in_specs=[anywhere, hbm, hbm, anywhere, anywhere, anywhere],
        out_specs=(vmem, vmem, vmem),
        scratch_shapes=[
            pltpu.VMEM((n, width, width, chans), features.dtype),
            pltpu.SMEM(labels.shape, labels.dtype),
            pltpu.SMEM(subset_ids.shape, subset_ids.dtype),
            pltpu.VMEM(conv1_weight.shape[1:], conv1_weight.dtype),
            pltpu.VMEM(conv2_weight.shape[1:], conv2_weight.dtype),
            pltpu.VMEM(head.shape, head.dtype),
            pltpu.VMEM((GROUP * width * width, offsets * chans), features.dtype),
            pltpu.VMEM((n, 2, LANES), jnp.float32),
            pltpu.VMEM((n, 2, LANES), jnp.float32),
            pltpu.SemaphoreType.DMA((2,)),
            pltpu.SemaphoreType.DMA,
            pltpu.SemaphoreType.DMA((offsets,)),
            pltpu.SemaphoreType.DMA((offsets,)),
            pltpu.SemaphoreType.DMA,
            pltpu.SemaphoreType.DMA((n,)),
            pltpu.SemaphoreType.DMA((n,)),
            pltpu.SemaphoreType.DMA((n,)),
            pltpu.SemaphoreType.DMA((n,)),
        ],
        compiler_params=pltpu.CompilerParams(
            collective_id=0, has_side_effects=True, vmem_limit_bytes=60 * 1024 * 1024
        ),
    )(features, labels, subset_ids, conv1_weight, conv2_weight, head)


def solution(mesh):
    in_specs = (
        P(("dp", "mp"), None, None, None),
        P("dp"),
        P("mp"),
        P("mp", None, None, None),
        P("mp", None, None, None),
        P("mp", None, None),
    )
    out_specs = (P(("dp", "mp"), None), P(("dp", "mp")), P(("dp", "mp")))
    return jax.shard_map(
        functools.partial(shards, mesh.shape["mp"]),
        mesh=mesh, in_specs=in_specs, out_specs=out_specs, check_vma=False,
    )
```

```python
import functools

import jax
import jax.numpy as jnp
from jax import lax
from jax.experimental import pallas as pl
from jax.experimental.pallas import tpu as pltpu
from jax.sharding import PartitionSpec as P

SUBSETS = 256
GROUP = 8
LANES = 128
MESH = pl.DeviceIdType.MESH


def kernel(
    n, feat_ref, labels_ref, ids_ref, w1_ref, w2_ref, head_ref,
    got,
    gathered, labels, ids, w1, w2, head, lhs, msg,
    small_sem, own_sem, w1_sem, w2_sem, head_sem, fsend, frecv, msend, mrecv,
):
    me = lax.axis_index("mp")
    width = feat_ref.shape[1]
    chans = feat_ref.shape[3]
    spots = width * width
    rows = GROUP * spots
    offsets = w1_ref.shape[1]
    classes = head_ref.shape[0]

    own = pltpu.make_async_copy(feat_ref.at[0], gathered.at[me], own_sem)
    own.start()
    small_copies = [
        pltpu.make_async_copy(labels_ref, labels, small_sem.at[0]),
        pltpu.make_async_copy(ids_ref, ids, small_sem.at[1]),
    ]
    for copy in small_copies:
        copy.start()
    w1_copies = [
        pltpu.make_async_copy(w1_ref.at[0, o], w1.at[o], w1_sem.at[o]) for o in range(offsets)
    ]
    w2_copies = [
        pltpu.make_async_copy(w2_ref.at[0, o], w2.at[o], w2_sem.at[o]) for o in range(offsets)
    ]
    head_copy = pltpu.make_async_copy(head_ref, head, head_sem)

    turn = 2 * lax.div(2 * me, n) - 1
    peers = [lax.rem(me + turn * j + n, n) for j in range(1, n)]
    barrier = pltpu.get_barrier_semaphore()
    for peer in peers:
        pl.semaphore_signal(barrier, inc=1, device_id={"mp": peer}, device_id_type=MESH)
    for copy in w1_copies:
        copy.start()
    for copy in w2_copies:
        copy.start()
    head_copy.start()

    r = lax.broadcasted_iota(jnp.int32, (rows, rows), 0)
    c = lax.broadcasted_iota(jnp.int32, (rows, rows), 1)
    source = lax.rem(r, GROUP) * spots + lax.div(r, GROUP)
    reorder = jnp.where(c == source, 1.0, 0.0).astype(jnp.bfloat16)
    sub = lax.broadcasted_iota(jnp.int32, (GROUP, 1), 0)
    for copy in small_copies:
        copy.wait()
    identity = ids[0].astype(jnp.float32)
    for t in range(n):
        msg[t, 1:2, :] = jnp.full((1, LANES), identity, jnp.float32)

    own.wait()
    pl.semaphore_wait(barrier, n - 1)
    feature_sends = []
    for j, peer in enumerate(peers):
        copy = pltpu.make_async_remote_copy(
            src_ref=gathered.at[me], dst_ref=gathered.at[me],
            send_sem=fsend.at[j], recv_sem=frecv.at[me],
            device_id={"mp": peer}, device_id_type=MESH,
        )
        copy.start()
        feature_sends.append(copy)

    for copy in w1_copies:
        copy.wait()
    for copy in w2_copies:
        copy.wait()
    head_copy.wait()
    for peer in peers:
        pltpu.make_async_remote_copy(
            src_ref=gathered.at[peer], dst_ref=gathered.at[peer],
            send_sem=fsend.at[0], recv_sem=frecv.at[peer],
            device_id={"mp": peer}, device_id_type=MESH,
        ).wait_recv()

    def convolve(grid, kernel_ref):
        blank = jnp.zeros((GROUP, chans), jnp.float32)
        for o in range(offsets):
            dy, dx = o // 3 - 1, o % 3 - 1
            blocks = []
            for y in range(width):
                for x in range(width):
                    inside = 0 <= y + dy < width and 0 <= x + dx < width
                    q = ((y + dy) * width + x + dx) * GROUP
                    blocks.append(grid[q : q + GROUP] if inside else blank)
            lhs[:, o * chans : (o + 1) * chans] = jnp.concatenate(blocks, 0).astype(jnp.bfloat16)
        return jnp.dot(
            lhs[...],
            kernel_ref[...].reshape(offsets * chans, chans),
            preferred_element_type=jnp.float32,
        )

    def group(first):
        raw = gathered[pl.ds(first, GROUP)].astype(jnp.float32).reshape(rows, chans)
        grid = jnp.dot(reorder, raw.astype(jnp.bfloat16), preferred_element_type=jnp.float32)
        hidden = jnp.maximum(convolve(grid, w1), 0.0)
        block = grid + jnp.maximum(convolve(hidden, w2), 0.0)
        pooled = block[:GROUP]
        for p in range(1, spots):
            pooled = jnp.maximum(pooled, block[p * GROUP : (p + 1) * GROUP])
        label = jnp.zeros((GROUP, 1), jnp.int32)
        for t in range(GROUP):
            label = jnp.where(sub == t, labels[first + t], label)
        correct = jnp.zeros((GROUP, 1), jnp.float32)
        rival = jnp.full((GROUP, 1), -1e30, jnp.float32)
        for k in range(classes):
            logit = jnp.sum(pooled * head[k], axis=1, keepdims=True)
            correct = jnp.where(label == k, logit, correct)
            rival = jnp.where(label == k, rival, jnp.maximum(rival, logit))
        margin = jnp.broadcast_to(correct - rival, (GROUP, LANES))
        for t in range(GROUP):
            msg[first + t, 0:1, :] = margin[t : t + 1]

    if n == GROUP:
        group(0)
    else:
        pl.loop(0, n // GROUP)(lambda g: group(g * GROUP))

    margin_sends = []
    for j, peer in enumerate(peers):
        copy = pltpu.make_async_remote_copy(
            src_ref=msg.at[peer], dst_ref=got.at[me],
            send_sem=msend.at[j], recv_sem=mrecv.at[me],
            device_id={"mp": peer}, device_id_type=MESH,
        )
        copy.start()
        margin_sends.append(copy)
    got[me] = msg[me]
    for copy in feature_sends:
        copy.wait_send()
    for copy in margin_sends:
        copy.wait_send()
    for peer in peers:
        pltpu.make_async_remote_copy(
            src_ref=msg.at[peer], dst_ref=got.at[peer],
            send_sem=msend.at[0], recv_sem=mrecv.at[peer],
            device_id={"mp": peer}, device_id_type=MESH,
        ).wait_recv()


def finish(got, data_ref, mean_ref, norm_ref):
    n = got.shape[0]
    total = got[0, 0:1, :]
    for m in range(1, n):
        total = total + got[m, 0:1, :]
    mean = total / n
    spread = jnp.zeros_like(mean)
    for m in range(n):
        centred = got[m, 0:1, :] - mean
        spread = spread + centred * centred
    norm = jnp.sqrt(1.0 + spread / n)
    lane = lax.broadcasted_iota(jnp.int32, (1, LANES), 1).astype(jnp.float32)
    for start in range(0, SUBSETS, LANES):
        acc = jnp.zeros((1, LANES), jnp.float32)
        for m in range(n):
            scaled = (got[m, 0:1, :] - mean) / norm
            acc = acc + jnp.where(got[m, 1:2, :] == lane + start, scaled, 0.0)
        data_ref[:, start : start + LANES] = acc
    mean_ref[...] = mean[0, :1]
    norm_ref[...] = norm[0, :1]


def shards(n, features, labels, subset_ids, conv1_weight, conv2_weight, head_weight):
    width, chans = features.shape[1], features.shape[3]
    offsets = conv1_weight.shape[1]
    assert features.shape[0] == 1 and conv1_weight.shape[0] == 1 and n % GROUP == 0
    head = jnp.transpose(head_weight, (2, 0, 1))
    anywhere = pl.BlockSpec(memory_space=pl.ANY)
    hbm = pl.BlockSpec(memory_space=pltpu.HBM)
    vmem = pl.BlockSpec(memory_space=pltpu.VMEM)
    got = pl.pallas_call(
        functools.partial(kernel, n),
        out_shape=pltpu.VMEM((n, 2, LANES), jnp.float32),
        in_specs=[anywhere, hbm, hbm, anywhere, anywhere, anywhere],
        out_specs=vmem,
        scratch_shapes=[
            pltpu.VMEM((n, width, width, chans), features.dtype),
            pltpu.SMEM(labels.shape, labels.dtype),
            pltpu.SMEM(subset_ids.shape, subset_ids.dtype),
            pltpu.VMEM(conv1_weight.shape[1:], conv1_weight.dtype),
            pltpu.VMEM(conv2_weight.shape[1:], conv2_weight.dtype),
            pltpu.VMEM(head.shape, head.dtype),
            pltpu.VMEM((GROUP * width * width, offsets * chans), features.dtype),
            pltpu.VMEM((n, 2, LANES), jnp.float32),
            pltpu.SemaphoreType.DMA((2,)),
            pltpu.SemaphoreType.DMA,
            pltpu.SemaphoreType.DMA((offsets,)),
            pltpu.SemaphoreType.DMA((offsets,)),
            pltpu.SemaphoreType.DMA,
            pltpu.SemaphoreType.DMA((n,)),
            pltpu.SemaphoreType.DMA((n,)),
            pltpu.SemaphoreType.DMA((n,)),
            pltpu.SemaphoreType.DMA((n,)),
        ],
        compiler_params=pltpu.CompilerParams(
            collective_id=0, has_side_effects=True, vmem_limit_bytes=60 * 1024 * 1024
        ),
    )(features, labels, subset_ids, conv1_weight, conv2_weight, head)
    return pl.pallas_call(
        finish,
        out_shape=(
            jax.ShapeDtypeStruct((1, SUBSETS), jnp.float32),
            jax.ShapeDtypeStruct((1,), jnp.float32),
            jax.ShapeDtypeStruct((1,), jnp.float32),
        ),
        in_specs=[vmem],
        out_specs=(vmem, vmem, vmem),
    )(pltpu.with_memory_space_constraint(got, pltpu.VMEM))


def solution(mesh):
    in_specs = (
        P(("dp", "mp"), None, None, None),
        P("dp"),
        P("mp"),
        P("mp", None, None, None),
        P("mp", None, None, None),
        P("mp", None, None),
    )
    out_specs = (P(("dp", "mp"), None), P(("dp", "mp")), P(("dp", "mp")))
    return jax.shard_map(
        functools.partial(shards, mesh.shape["mp"]),
        mesh=mesh, in_specs=in_specs, out_specs=out_specs, check_vma=False,
    )
```

```python
import functools

import jax
import jax.numpy as jnp
from jax import lax
from jax.experimental import pallas as pl
from jax.experimental.pallas import tpu as pltpu
from jax.sharding import PartitionSpec as P

SUBSETS = 256
GROUP = 8
LANES = 128
MESH = pl.DeviceIdType.MESH


def kernel(
    n, feat_ref, labels_ref, ids_ref, w1_ref, w2_ref, head_ref,
    got,
    mine, gathered, named, asked, labels, ids, w1, w2, head, lhs, msg,
    small_sem, own_sem, name_sems, w1_sem, w2_sem, head_sem, fsend, frecv, msend, mrecv,
):
    me = lax.axis_index("mp")
    dp = lax.axis_index("dp")
    other = dp + 1 - 2 * lax.rem(dp, 2)
    width = feat_ref.shape[1]
    chans = feat_ref.shape[3]
    spots = width * width
    rows = GROUP * spots
    offsets = w1_ref.shape[1]
    classes = head_ref.shape[0]

    own = pltpu.make_async_copy(feat_ref.at[0], mine, own_sem)
    own.start()
    small_copies = [
        pltpu.make_async_copy(labels_ref, named, small_sem.at[0]),
        pltpu.make_async_copy(ids_ref, ids, small_sem.at[1]),
    ]
    for copy in small_copies:
        copy.start()
    w1_copies = [
        pltpu.make_async_copy(w1_ref.at[0, o], w1.at[o], w1_sem.at[o]) for o in range(offsets)
    ]
    w2_copies = [
        pltpu.make_async_copy(w2_ref.at[0, o], w2.at[o], w2_sem.at[o]) for o in range(offsets)
    ]
    head_copy = pltpu.make_async_copy(head_ref, head, head_sem)

    turn = 2 * lax.div(2 * me, n) - 1
    peers = [lax.rem(me + turn * j + n, n) for j in range(1, n)] + [me]
    barrier = pltpu.get_barrier_semaphore()
    for peer in peers:
        pl.semaphore_signal(barrier, inc=1, device_id={"mp": peer, "dp": other}, device_id_type=MESH)
    for copy in w1_copies:
        copy.start()
    for copy in w2_copies:
        copy.start()
    head_copy.start()

    r = lax.broadcasted_iota(jnp.int32, (rows, rows), 0)
    c = lax.broadcasted_iota(jnp.int32, (rows, rows), 1)
    source = lax.rem(r, GROUP) * spots + lax.div(r, GROUP)
    reorder = jnp.where(c == source, 1.0, 0.0).astype(jnp.bfloat16)
    sub = lax.broadcasted_iota(jnp.int32, (GROUP, 1), 0)
    for copy in small_copies:
        copy.wait()
    identity = ids[0].astype(jnp.float32)
    for t in range(n):
        msg[t, 1:2, :] = jnp.full((1, LANES), identity, jnp.float32)

    own.wait()
    pl.semaphore_wait(barrier, n)
    feature_sends = []
    for j, peer in enumerate(peers):
        copy = pltpu.make_async_remote_copy(
            src_ref=mine, dst_ref=gathered.at[me],
            send_sem=fsend.at[j], recv_sem=frecv.at[me],
            device_id={"mp": peer, "dp": other}, device_id_type=MESH,
        )
        copy.start()
        feature_sends.append(copy)
    name_send = pltpu.make_async_remote_copy(
        src_ref=named, dst_ref=asked,
        send_sem=name_sems.at[0], recv_sem=name_sems.at[1],
        device_id={"mp": me, "dp": other}, device_id_type=MESH,
    )
    name_send.start()

    for copy in w1_copies:
        copy.wait()
    for copy in w2_copies:
        copy.wait()
    head_copy.wait()
    name_send.wait()
    asked_copy = pltpu.make_async_copy(asked, labels, small_sem.at[0])
    asked_copy.start()
    asked_copy.wait()
    for peer in peers:
        pltpu.make_async_remote_copy(
            src_ref=mine, dst_ref=gathered.at[peer],
            send_sem=fsend.at[0], recv_sem=frecv.at[peer],
            device_id={"mp": peer, "dp": other}, device_id_type=MESH,
        ).wait_recv()

    def convolve(grid, kernel_ref):
        blank = jnp.zeros((GROUP, chans), jnp.float32)
        for o in range(offsets):
            dy, dx = o // 3 - 1, o % 3 - 1
            blocks = []
            for y in range(width):
                for x in range(width):
                    inside = 0 <= y + dy < width and 0 <= x + dx < width
                    q = ((y + dy) * width + x + dx) * GROUP
                    blocks.append(grid[q : q + GROUP] if inside else blank)
            lhs[:, o * chans : (o + 1) * chans] = jnp.concatenate(blocks, 0).astype(jnp.bfloat16)
        return jnp.dot(
            lhs[...],
            kernel_ref[...].reshape(offsets * chans, chans),
            preferred_element_type=jnp.float32,
        )

    def group(first):
        raw = gathered[pl.ds(first, GROUP)].astype(jnp.float32).reshape(rows, chans)
        grid = jnp.dot(reorder, raw.astype(jnp.bfloat16), preferred_element_type=jnp.float32)
        hidden = jnp.maximum(convolve(grid, w1), 0.0)
        block = grid + jnp.maximum(convolve(hidden, w2), 0.0)
        pooled = block[:GROUP]
        for p in range(1, spots):
            pooled = jnp.maximum(pooled, block[p * GROUP : (p + 1) * GROUP])
        label = jnp.zeros((GROUP, 1), jnp.int32)
        for t in range(GROUP):
            label = jnp.where(sub == t, labels[first + t], label)
        correct = jnp.zeros((GROUP, 1), jnp.float32)
        rival = jnp.full((GROUP, 1), -1e30, jnp.float32)
        for k in range(classes):
            logit = jnp.sum(pooled * head[k], axis=1, keepdims=True)
            correct = jnp.where(label == k, logit, correct)
            rival = jnp.where(label == k, rival, jnp.maximum(rival, logit))
        margin = jnp.broadcast_to(correct - rival, (GROUP, LANES))
        for t in range(GROUP):
            msg[first + t, 0:1, :] = margin[t : t + 1]

    if n == GROUP:
        group(0)
    else:
        pl.loop(0, n // GROUP)(lambda g: group(g * GROUP))

    margin_sends = []
    for j, peer in enumerate(peers):
        copy = pltpu.make_async_remote_copy(
            src_ref=msg.at[peer], dst_ref=got.at[me],
            send_sem=msend.at[j], recv_sem=mrecv.at[me],
            device_id={"mp": peer, "dp": other}, device_id_type=MESH,
        )
        copy.start()
        margin_sends.append(copy)
    for copy in feature_sends:
        copy.wait_send()
    for copy in margin_sends:
        copy.wait_send()
    for peer in peers:
        pltpu.make_async_remote_copy(
            src_ref=msg.at[peer], dst_ref=got.at[peer],
            send_sem=msend.at[0], recv_sem=mrecv.at[peer],
            device_id={"mp": peer, "dp": other}, device_id_type=MESH,
        ).wait_recv()


def finish(got, data_ref, mean_ref, norm_ref):
    n = got.shape[0]
    total = got[0, 0:1, :]
    for m in range(1, n):
        total = total + got[m, 0:1, :]
    mean = total / n
    spread = jnp.zeros_like(mean)
    for m in range(n):
        centred = got[m, 0:1, :] - mean
        spread = spread + centred * centred
    norm = jnp.sqrt(1.0 + spread / n)
    lane = lax.broadcasted_iota(jnp.int32, (1, LANES), 1).astype(jnp.float32)
    for start in range(0, SUBSETS, LANES):
        acc = jnp.zeros((1, LANES), jnp.float32)
        for m in range(n):
            scaled = (got[m, 0:1, :] - mean) / norm
            acc = acc + jnp.where(got[m, 1:2, :] == lane + start, scaled, 0.0)
        data_ref[:, start : start + LANES] = acc
    mean_ref[...] = mean[0, :1]
    norm_ref[...] = norm[0, :1]


def shards(n, features, labels, subset_ids, conv1_weight, conv2_weight, head_weight):
    width, chans = features.shape[1], features.shape[3]
    offsets = conv1_weight.shape[1]
    assert features.shape[0] == 1 and conv1_weight.shape[0] == 1 and n % GROUP == 0
    head = jnp.transpose(head_weight, (2, 0, 1))
    anywhere = pl.BlockSpec(memory_space=pl.ANY)
    hbm = pl.BlockSpec(memory_space=pltpu.HBM)
    vmem = pl.BlockSpec(memory_space=pltpu.VMEM)
    got = pl.pallas_call(
        functools.partial(kernel, n),
        out_shape=pltpu.VMEM((n, 2, LANES), jnp.float32),
        in_specs=[anywhere, hbm, hbm, anywhere, anywhere, anywhere],
        out_specs=vmem,
        scratch_shapes=[
            pltpu.VMEM((width, width, chans), features.dtype),
            pltpu.VMEM((n, width, width, chans), features.dtype),
            pltpu.VMEM(labels.shape, labels.dtype),
            pltpu.VMEM(labels.shape, labels.dtype),
            pltpu.SMEM(labels.shape, labels.dtype),
            pltpu.SMEM(subset_ids.shape, subset_ids.dtype),
            pltpu.VMEM(conv1_weight.shape[1:], conv1_weight.dtype),
            pltpu.VMEM(conv2_weight.shape[1:], conv2_weight.dtype),
            pltpu.VMEM(head.shape, head.dtype),
            pltpu.VMEM((GROUP * width * width, offsets * chans), features.dtype),
            pltpu.VMEM((n, 2, LANES), jnp.float32),
            pltpu.SemaphoreType.DMA((2,)),
            pltpu.SemaphoreType.DMA,
            pltpu.SemaphoreType.DMA((2,)),
            pltpu.SemaphoreType.DMA((offsets,)),
            pltpu.SemaphoreType.DMA((offsets,)),
            pltpu.SemaphoreType.DMA,
            pltpu.SemaphoreType.DMA((n,)),
            pltpu.SemaphoreType.DMA((n,)),
            pltpu.SemaphoreType.DMA((n,)),
            pltpu.SemaphoreType.DMA((n,)),
        ],
        compiler_params=pltpu.CompilerParams(
            collective_id=0, has_side_effects=True, vmem_limit_bytes=60 * 1024 * 1024
        ),
    )(features, labels, subset_ids, conv1_weight, conv2_weight, head)
    return pl.pallas_call(
        finish,
        out_shape=(
            jax.ShapeDtypeStruct((1, SUBSETS), jnp.float32),
            jax.ShapeDtypeStruct((1,), jnp.float32),
            jax.ShapeDtypeStruct((1,), jnp.float32),
        ),
        in_specs=[vmem],
        out_specs=(vmem, vmem, vmem),
    )(pltpu.with_memory_space_constraint(got, pltpu.VMEM))


def solution(mesh):
    in_specs = (
        P(("dp", "mp"), None, None, None),
        P("dp"),
        P("mp"),
        P("mp", None, None, None),
        P("mp", None, None, None),
        P("mp", None, None),
    )
    out_specs = (P(("dp", "mp"), None), P(("dp", "mp")), P(("dp", "mp")))
    assert mesh.shape["dp"] % 2 == 0
    return jax.shard_map(
        functools.partial(shards, mesh.shape["mp"]),
        mesh=mesh, in_specs=in_specs, out_specs=out_specs, check_vma=False,
    )
```

```python
import functools

import jax
import jax.numpy as jnp
from jax import lax
from jax.experimental import pallas as pl
from jax.experimental.pallas import tpu as pltpu
from jax.sharding import PartitionSpec as P

SUBSETS = 256
GROUP = 8
LANES = 128
MESH = pl.DeviceIdType.MESH


def kernel(
    n, feat_ref, labels_ref, ids_ref, w1_ref, w2_ref, head_ref,
    got,
    mine, gathered, named, asked, labels, ids, w1, w2, head, lhs, msg,
    small_sem, own_sem, name_sems, w1_sem, w2_sem, head_sem, fsend, frecv, msend, mrecv,
):
    me = lax.axis_index("mp")
    dp = lax.axis_index("dp")
    other = dp + 1 - 2 * lax.rem(dp, 2)
    width = feat_ref.shape[1]
    chans = feat_ref.shape[3]
    spots = width * width
    rows = GROUP * spots
    offsets = w1_ref.shape[1]
    classes = head_ref.shape[0]

    own = pltpu.make_async_copy(feat_ref.at[0], mine, own_sem)
    own.start()
    small_copies = [
        pltpu.make_async_copy(labels_ref, named, small_sem.at[0]),
        pltpu.make_async_copy(ids_ref, ids, small_sem.at[1]),
    ]
    for copy in small_copies:
        copy.start()
    w1_copies = [
        pltpu.make_async_copy(w1_ref.at[0, o], w1.at[o], w1_sem.at[o]) for o in range(offsets)
    ]
    w2_copies = [
        pltpu.make_async_copy(w2_ref.at[0, o], w2.at[o], w2_sem.at[o]) for o in range(offsets)
    ]
    head_copy = pltpu.make_async_copy(head_ref, head, head_sem)

    turn = 2 * lax.div(2 * me, n) - 1
    peers = [lax.rem(me + turn * j + n, n) for j in range(1, n)] + [me]
    barrier = pltpu.get_barrier_semaphore()
    for peer in peers:
        pl.semaphore_signal(barrier, inc=1, device_id={"mp": peer, "dp": other}, device_id_type=MESH)
    for copy in w1_copies:
        copy.start()
    for copy in w2_copies:
        copy.start()
    head_copy.start()

    r = lax.broadcasted_iota(jnp.int32, (rows, rows), 0)
    c = lax.broadcasted_iota(jnp.int32, (rows, rows), 1)
    source = lax.rem(r, GROUP) * spots + lax.div(r, GROUP)
    reorder = jnp.where(c == source, 1.0, 0.0).astype(jnp.bfloat16)
    sub = lax.broadcasted_iota(jnp.int32, (GROUP, 1), 0)
    for copy in small_copies:
        copy.wait()
    identity = ids[0].astype(jnp.float32)
    for t in range(n):
        msg[t, 1:2, :] = jnp.full((1, LANES), identity, jnp.float32)

    own.wait()
    pl.semaphore_wait(barrier, n)
    feature_sends = []
    for j, peer in enumerate(peers):
        copy = pltpu.make_async_remote_copy(
            src_ref=mine, dst_ref=gathered.at[me],
            send_sem=fsend.at[j], recv_sem=frecv.at[me],
            device_id={"mp": peer, "dp": other}, device_id_type=MESH,
        )
        copy.start()
        feature_sends.append(copy)
    name_send = pltpu.make_async_remote_copy(
        src_ref=named, dst_ref=asked,
        send_sem=name_sems.at[0], recv_sem=name_sems.at[1],
        device_id={"mp": me, "dp": other}, device_id_type=MESH,
    )
    name_send.start()

    for copy in w1_copies:
        copy.wait()
    for copy in w2_copies:
        copy.wait()
    head_copy.wait()
    name_send.wait()
    asked_copy = pltpu.make_async_copy(asked, labels, small_sem.at[0])
    asked_copy.start()
    for peer in peers:
        pltpu.make_async_remote_copy(
            src_ref=mine, dst_ref=gathered.at[peer],
            send_sem=fsend.at[0], recv_sem=frecv.at[peer],
            device_id={"mp": peer, "dp": other}, device_id_type=MESH,
        ).wait_recv()

    asked_copy.wait()

    def convolve(grid, kernel_ref):
        blank = jnp.zeros((GROUP, chans), jnp.float32)
        for o in range(offsets):
            dy, dx = o // 3 - 1, o % 3 - 1
            blocks = []
            for y in range(width):
                for x in range(width):
                    inside = 0 <= y + dy < width and 0 <= x + dx < width
                    q = ((y + dy) * width + x + dx) * GROUP
                    blocks.append(grid[q : q + GROUP] if inside else blank)
            lhs[:, o * chans : (o + 1) * chans] = jnp.concatenate(blocks, 0).astype(jnp.bfloat16)
        return jnp.dot(
            lhs[...],
            kernel_ref[...].reshape(offsets * chans, chans),
            preferred_element_type=jnp.float32,
        )

    def group(first):
        raw = gathered[pl.ds(first, GROUP)].astype(jnp.float32).reshape(rows, chans)
        grid = jnp.dot(reorder, raw.astype(jnp.bfloat16), preferred_element_type=jnp.float32)
        hidden = jnp.maximum(convolve(grid, w1), 0.0)
        block = grid + jnp.maximum(convolve(hidden, w2), 0.0)
        pooled = block[:GROUP]
        for p in range(1, spots):
            pooled = jnp.maximum(pooled, block[p * GROUP : (p + 1) * GROUP])
        label = jnp.zeros((GROUP, 1), jnp.int32)
        for t in range(GROUP):
            label = jnp.where(sub == t, labels[first + t], label)
        correct = jnp.zeros((GROUP, 1), jnp.float32)
        rival = jnp.full((GROUP, 1), -1e30, jnp.float32)
        for k in range(classes):
            logit = jnp.sum(pooled * head[k], axis=1, keepdims=True)
            correct = jnp.where(label == k, logit, correct)
            rival = jnp.where(label == k, rival, jnp.maximum(rival, logit))
        margin = jnp.broadcast_to(correct - rival, (GROUP, LANES))
        for t in range(GROUP):
            msg[first + t, 0:1, :] = margin[t : t + 1]

    if n == GROUP:
        group(0)
    else:
        pl.loop(0, n // GROUP)(lambda g: group(g * GROUP))

    margin_sends = []
    for j, peer in enumerate(peers):
        copy = pltpu.make_async_remote_copy(
            src_ref=msg.at[peer], dst_ref=got.at[me],
            send_sem=msend.at[j], recv_sem=mrecv.at[me],
            device_id={"mp": peer, "dp": other}, device_id_type=MESH,
        )
        copy.start()
        margin_sends.append(copy)
    for copy in feature_sends:
        copy.wait_send()
    for copy in margin_sends:
        copy.wait_send()
    for peer in peers:
        pltpu.make_async_remote_copy(
            src_ref=msg.at[peer], dst_ref=got.at[peer],
            send_sem=msend.at[0], recv_sem=mrecv.at[peer],
            device_id={"mp": peer, "dp": other}, device_id_type=MESH,
        ).wait_recv()


def finish(got, data_ref, mean_ref, norm_ref):
    n = got.shape[0]
    total = got[0, 0:1, :]
    for m in range(1, n):
        total = total + got[m, 0:1, :]
    mean = total / n
    spread = jnp.zeros_like(mean)
    for m in range(n):
        centred = got[m, 0:1, :] - mean
        spread = spread + centred * centred
    norm = jnp.sqrt(1.0 + spread / n)
    lane = lax.broadcasted_iota(jnp.int32, (1, LANES), 1).astype(jnp.float32)
    scaled = [(got[m, 0:1, :] - mean) / norm for m in range(n)]
    for start in range(0, SUBSETS, LANES):
        acc = jnp.zeros((1, LANES), jnp.float32)
        for m in range(n):
            acc = acc + jnp.where(got[m, 1:2, :] == lane + start, scaled[m], 0.0)
        data_ref[:, start : start + LANES] = acc
    mean_ref[...] = mean[0, :1]
    norm_ref[...] = norm[0, :1]


def shards(n, features, labels, subset_ids, conv1_weight, conv2_weight, head_weight):
    width, chans = features.shape[1], features.shape[3]
    offsets = conv1_weight.shape[1]
    assert features.shape[0] == 1 and conv1_weight.shape[0] == 1 and n % GROUP == 0
    head = jnp.transpose(head_weight, (2, 0, 1))
    anywhere = pl.BlockSpec(memory_space=pl.ANY)
    hbm = pl.BlockSpec(memory_space=pltpu.HBM)
    vmem = pl.BlockSpec(memory_space=pltpu.VMEM)
    got = pl.pallas_call(
        functools.partial(kernel, n),
        out_shape=pltpu.VMEM((n, 2, LANES), jnp.float32),
        in_specs=[anywhere, hbm, hbm, anywhere, anywhere, anywhere],
        out_specs=vmem,
        scratch_shapes=[
            pltpu.VMEM((width, width, chans), features.dtype),
            pltpu.VMEM((n, width, width, chans), features.dtype),
            pltpu.VMEM(labels.shape, labels.dtype),
            pltpu.VMEM(labels.shape, labels.dtype),
            pltpu.SMEM(labels.shape, labels.dtype),
            pltpu.SMEM(subset_ids.shape, subset_ids.dtype),
            pltpu.VMEM(conv1_weight.shape[1:], conv1_weight.dtype),
            pltpu.VMEM(conv2_weight.shape[1:], conv2_weight.dtype),
            pltpu.VMEM(head.shape, head.dtype),
            pltpu.VMEM((GROUP * width * width, offsets * chans), features.dtype),
            pltpu.VMEM((n, 2, LANES), jnp.float32),
            pltpu.SemaphoreType.DMA((2,)),
            pltpu.SemaphoreType.DMA,
            pltpu.SemaphoreType.DMA((2,)),
            pltpu.SemaphoreType.DMA((offsets,)),
            pltpu.SemaphoreType.DMA((offsets,)),
            pltpu.SemaphoreType.DMA,
            pltpu.SemaphoreType.DMA((n,)),
            pltpu.SemaphoreType.DMA((n,)),
            pltpu.SemaphoreType.DMA((n,)),
            pltpu.SemaphoreType.DMA((n,)),
        ],
        compiler_params=pltpu.CompilerParams(
            collective_id=0, has_side_effects=True, vmem_limit_bytes=60 * 1024 * 1024
        ),
    )(features, labels, subset_ids, conv1_weight, conv2_weight, head)
    return pl.pallas_call(
        finish,
        out_shape=(
            jax.ShapeDtypeStruct((1, SUBSETS), jnp.float32),
            jax.ShapeDtypeStruct((1,), jnp.float32),
            jax.ShapeDtypeStruct((1,), jnp.float32),
        ),
        in_specs=[vmem],
        out_specs=(vmem, vmem, vmem),
    )(pltpu.with_memory_space_constraint(got, pltpu.VMEM))


def solution(mesh):
    in_specs = (
        P(("dp", "mp"), None, None, None),
        P("dp"),
        P("mp"),
        P("mp", None, None, None),
        P("mp", None, None, None),
        P("mp", None, None),
    )
    out_specs = (P(("dp", "mp"), None), P(("dp", "mp")), P(("dp", "mp")))
    assert mesh.shape["dp"] % 2 == 0
    return jax.shard_map(
        functools.partial(shards, mesh.shape["mp"]),
        mesh=mesh, in_specs=in_specs, out_specs=out_specs, check_vma=False,
    )
```
